128 devices in a mesh: kx: 4 (over z_lo, core), ky: 4 (over x), kz: 8 (over z_hi, y).
Axes of the slice: x: 4, y: 4, z: 4 (z_hi: 2, z_lo: 2; z = z_hi * 2 + z_lo), core: 2. Of those that a mesh axis runs over, the one named last changes fastest.
Arguments:
- offsets: int32 [12, 3], replicated, may hold values from -1 to 1, as said below
- gauge: float32 [2, 4, 4, 16, 256, 256], P(None, 'kx', 'ky', 'kz'), may hold values from -1 to 1, as said below
- intersections: bfloat16 [12, 2, 4, 4, 16, 256, 256], P(None, None, 'kx', 'ky', 'kz'), may hold values from -1 to 1
Outputs:
- new_gauge: float32 [2, 4, 4, 16, 256, 256], P(None, 'kx', 'ky', 'kz')
- centres: float32 [3, 256], replicated
- spread: float32 [], replicated
The draws below stay inside these ranges and needn't reach their ends.
Inputs may be any that keep to these rules, and one draw needn't show every extreme that they name: `offsets`: the 12 rows are the twelve distinct vectors with two entries of magnitude one and one entry zero, each once. `gauge`: every 256 x 256 complex matrix of it is unitary to float32 rounding.
All inputs are finite; a program needn't handle non-finite values.
Results may differ from the reference program's by a relative error of at most 0.0068.
Values may be sent and summed in bfloat16 or wider, within the bound.
No kernel may reach another device: no remote copies, remote signals or barrier semaphores. Data moves between devices by JAX's collectives and lax.ppermute only.
A program may use at most 192 MiB of HBM per device.

```python
import math
import jax
import jax.numpy as jnp
import numpy as np
from jax import lax

NW = 256
NB = 12
TERMS = 12
NKX = 4
NKY = 4
NKZ = 16


def draw_offsets(key, part):
    table = np.array([[1, 1, 0], [1, -1, 0], [-1, 1, 0], [-1, -1, 0], [1, 0, 1], [1, 0, -1], [-1, 0, 1], [-1, 0, -1], [0, 1, 1], [0, 1, -1], [0, -1, 1], [0, -1, -1]], dtype=np.int32)
    order = jax.random.permutation(jax.random.fold_in(key, 11), NB)
    return jnp.asarray(table)[order]


def pair_product(left_real, left_imag, right_real, right_imag):
    highest = lax.Precision.HIGHEST
    real = jnp.matmul(left_real, right_real, precision=highest) - jnp.matmul(left_imag, right_imag, precision=highest)
    imag = jnp.matmul(left_real, right_imag, precision=highest) + jnp.matmul(left_imag, right_real, precision=highest)
    return (real, imag)


def draw_gauge(key, part):
    shape = (NKX, NKY, NKZ, NW, NW)
    first_key = jax.random.fold_in(key, 21)
    second_key = jax.random.fold_in(key, 22)
    scale = 0.7 / math.sqrt(NW)
    raw_real = jax.random.normal(first_key, shape, jnp.float32) * scale
    raw_imag = jax.random.normal(second_key, shape, jnp.float32) * scale
    quarter_real = 0.125 * (raw_real - jnp.swapaxes(raw_real, -1, -2))
    quarter_imag = 0.125 * (raw_imag + jnp.swapaxes(raw_imag, -1, -2))
    ident = jnp.broadcast_to(jnp.eye(NW, dtype=jnp.float32), shape)
    term_real, term_imag = (ident, jnp.zeros(shape, jnp.float32))
    total_real, total_imag = (term_real, term_imag)
    for order in range(1, 7):
        term_real, term_imag = pair_product(term_real, term_imag, quarter_real, quarter_imag)
        term_real = term_real / order
        term_imag = term_imag / order
        total_real = total_real + term_real
        total_imag = total_imag + term_imag
    for repeat in range(2):
        total_real, total_imag = pair_product(total_real, total_imag, total_real, total_imag)
    return jnp.stack([total_real, total_imag])


def draw_intersections(key, part):
    shape = (NB, NKX, NKY, NKZ, NW, NW)
    diag_shape = (NB, NKX, NKY, NKZ, NW)
    scale = 0.3 / math.sqrt(NW)
    index_x = jnp.arange(NKX, dtype=jnp.float32)[:, None, None]
    index_y = jnp.arange(NKY, dtype=jnp.float32)[None, :, None]
    index_z = jnp.arange(NKZ, dtype=jnp.float32)[None, None, :]
    flat = index_x * (NKY * NKZ) + index_y * NKZ + index_z
    position = (flat / max(NKX * NKY * NKZ - 1, 1))[None, :, :, :, None]
    off_real = jnp.clip(jax.random.normal(jax.random.fold_in(key, 31), shape, jnp.float32), -4.0, 4.0) * scale
    off_imag = jnp.clip(jax.random.normal(jax.random.fold_in(key, 32), shape, jnp.float32), -4.0, 4.0) * scale
    reach = 0.25 + 0.6 * position
    lowest = 0.7 - 0.4 * position
    fraction = jax.random.uniform(jax.random.fold_in(key, 33), diag_shape, jnp.float32, 0.0, 1.0)
    magnitude = jnp.exp(jnp.log(lowest) * fraction)
    angle = jax.random.uniform(jax.random.fold_in(key, 34), diag_shape, jnp.float32, -1.0, 1.0) * reach
    eye = jnp.eye(NW, dtype=jnp.float32)
    real = off_real * (1.0 - eye) + eye * (magnitude * jnp.cos(angle))[..., None, :]
    imag = off_imag * (1.0 - eye) + eye * (magnitude * jnp.sin(angle))[..., None, :]
    return jnp.stack([real.astype(jnp.bfloat16), imag.astype(jnp.bfloat16)], axis=1)


def setup_inputs(seed: int = 0) -> dict:
    arg_keys = jax.random.split(jax.random.key(seed), 4)
    offsets = draw_offsets(jax.random.fold_in(arg_keys[3], 71), 0)
    gauge = draw_gauge(jax.random.fold_in(arg_keys[3], 71), 0)
    intersections = draw_intersections(jax.random.fold_in(arg_keys[3], 71), 0)
    return dict(offsets=offsets, gauge=gauge, intersections=intersections)


descent_step = 2.0
magnitude_floor = 0.25
highest = lax.Precision.HIGHEST


def transpose_last(matrix):
    return jnp.swapaxes(matrix, -1, -2)


def anti_hermitian(real, imag):
    return 0.5 * (real - transpose_last(real)), 0.5 * (imag + transpose_last(imag))


def skew_part(real, imag):
    return 0.5 * (imag - transpose_last(imag)), -0.5 * (real + transpose_last(real))


def complex_product(left, right):
    real = jnp.matmul(left[0], right[0], precision=highest) - jnp.matmul(left[1], right[1], precision=highest)
    imag = jnp.matmul(left[0], right[1], precision=highest) + jnp.matmul(left[1], right[0], precision=highest)
    return jnp.stack([real, imag])


def exponential(generator):
    size = generator.shape[-1]
    ident = jnp.broadcast_to(jnp.eye(size, dtype=jnp.float32), generator.shape[1:])
    initial = jnp.stack([ident, jnp.zeros_like(ident)])

    def advance(order, carry):
        term, total = carry
        term = complex_product(term, generator) / order.astype(jnp.float32)
        return term, total + term

    final = lax.fori_loop(1, TERMS + 1, advance, (initial, initial))
    return final[1]


def geometry(offsets, counts):
    spacing = jnp.array([2.0 * math.pi / counts[0], 2.0 * math.pi / counts[1], 2.0 * math.pi / counts[2]], jnp.float32)
    bvec = offsets.astype(jnp.float32) * spacing
    weights = 1.0 / (4.0 * jnp.sum(bvec * bvec, axis=1))
    return bvec, weights


def local_terms(m_real, m_imag, bvec, weights):
    diag_real = jnp.diagonal(m_real, axis1=-2, axis2=-1)
    diag_imag = jnp.diagonal(m_imag, axis1=-2, axis2=-1)
    phase = jnp.arctan2(diag_imag, diag_real)
    squared = diag_real * diag_real + diag_imag * diag_imag
    denom = jnp.maximum(squared, magnitude_floor)[..., None, :]
    col_real = diag_real[..., None, :]
    col_imag = diag_imag[..., None, :]
    rot_real = m_real * col_real + m_imag * col_imag
    rot_imag = m_imag * col_real - m_real * col_imag
    hat_real = rot_real / denom
    hat_imag = rot_imag / denom
    sum_rot_real = jnp.einsum("b,b...xy->...xy", weights, rot_real, precision=highest)
    sum_rot_imag = jnp.einsum("b,b...xy->...xy", weights, rot_imag, precision=highest)
    sum_tan_real = jnp.einsum("b,b...y,b...xy->...xy", weights, phase, hat_real, precision=highest)
    sum_tan_imag = jnp.einsum("b,b...y,b...xy->...xy", weights, phase, hat_imag, precision=highest)
    hsum_real = jnp.einsum("b,ba,b...xy->a...xy", weights, bvec, hat_real, precision=highest)
    hsum_imag = jnp.einsum("b,ba,b...xy->a...xy", weights, bvec, hat_imag, precision=highest)
    anti_real, anti_imag = anti_hermitian(sum_rot_real, sum_rot_imag)
    skew_real, skew_imag = skew_part(sum_tan_real, sum_tan_imag)
    return phase, squared, anti_real - skew_real, anti_imag - skew_imag, hsum_real, hsum_imag


def finish(base_real, base_imag, hsum_real, hsum_imag, centres, gauge_block):
    extra_real = jnp.einsum("a...xy,ay->...xy", hsum_real, centres, precision=highest)
    extra_imag = jnp.einsum("a...xy,ay->...xy", hsum_imag, centres, precision=highest)
    skew_real, skew_imag = skew_part(extra_real, extra_imag)
    generator = descent_step * 4.0 * jnp.stack([base_real - skew_real, base_imag - skew_imag])
    return complex_product(gauge_block, exponential(generator))


def reference(offsets, gauge, intersections):
    count_x, count_y, count_z, nbands = gauge.shape[1], gauge.shape[2], gauge.shape[3], gauge.shape[4]
    nvec = offsets.shape[0]
    total_k = count_x * count_y * count_z
    bvec, weights = geometry(offsets, (count_x, count_y, count_z))
    rounded = gauge.astype(jnp.bfloat16)
    zero_index = jnp.zeros((), jnp.int32)

    def point_index(flat):
        return flat // (count_y * count_z), (flat // count_z) % count_y, flat % count_z

    def first_pass(flat):
        index_x, index_y, index_z = point_index(flat)
        own_block = lax.dynamic_slice(rounded, (zero_index, index_x, index_y, index_z, zero_index, zero_index), (2, 1, 1, 1, nbands, nbands)).reshape(2, nbands, nbands).astype(jnp.float32)
        over_block = lax.dynamic_slice(intersections, (zero_index, zero_index, index_x, index_y, index_z, zero_index, zero_index), (nvec, 2, 1, 1, 1, nbands, nbands)).reshape(nvec, 2, nbands, nbands).astype(jnp.float32)
        left_real = jnp.einsum("ia,bie->bae", own_block[0], over_block[:, 0], precision=highest) + jnp.einsum("ia,bie->bae", own_block[1], over_block[:, 1], precision=highest)
        left_imag = jnp.einsum("ia,bie->bae", own_block[0], over_block[:, 1], precision=highest) - jnp.einsum("ia,bie->bae", own_block[1], over_block[:, 0], precision=highest)
        left_real = lax.optimization_barrier(left_real.astype(jnp.bfloat16)).astype(jnp.float32)
        left_imag = lax.optimization_barrier(left_imag.astype(jnp.bfloat16)).astype(jnp.float32)

        def fetch(vector):
            near_x = (index_x + vector[0]) % count_x
            near_y = (index_y + vector[1]) % count_y
            near_z = (index_z + vector[2]) % count_z
            block = lax.dynamic_slice(rounded, (zero_index, near_x, near_y, near_z, zero_index, zero_index), (2, 1, 1, 1, nbands, nbands))
            return block.reshape(2, nbands, nbands)

        neighbour = jax.vmap(fetch)(offsets).astype(jnp.float32)
        m_real = jnp.matmul(left_real, neighbour[:, 0], precision=highest) - jnp.matmul(left_imag, neighbour[:, 1], precision=highest)
        m_imag = jnp.matmul(left_real, neighbour[:, 1], precision=highest) + jnp.matmul(left_imag, neighbour[:, 0], precision=highest)
        return local_terms(m_real, m_imag, bvec, weights)

    points = jnp.arange(total_k, dtype=jnp.int32)
    phase, squared, base_real, base_imag, hsum_real, hsum_imag = lax.map(first_pass, points)
    centres = -jnp.einsum("b,ba,kbn->an", weights, bvec, phase, precision=highest) / total_k
    spread_terms = jnp.einsum("b,kbn->n", weights, 1.0 - squared + phase * phase, precision=highest)
    spread = jnp.sum(spread_terms) / total_k - jnp.sum(centres * centres)

    def second_pass(flat):
        index_x, index_y, index_z = point_index(flat)
        gauge_block = lax.dynamic_slice(gauge, (zero_index, index_x, index_y, index_z, zero_index, zero_index), (2, 1, 1, 1, nbands, nbands)).reshape(2, nbands, nbands)
        return finish(base_real[flat], base_imag[flat], hsum_real[flat], hsum_imag[flat], centres, gauge_block)

    updated = lax.map(second_pass, points)
    new_gauge = updated.reshape(count_x, count_y, count_z, 2, nbands, nbands).transpose(3, 0, 1, 2, 4, 5)
    return new_gauge, centres, spread
```

```python
import math

import jax
import jax.numpy as jnp
from jax import lax
from jax.experimental import pallas as pl
from jax.experimental.pallas import tpu as pltpu
from jax.sharding import PartitionSpec as P


TERMS = 12
STEP = 2.0
FLOOR = 0.25
F32 = jnp.float32
BF16 = jnp.bfloat16

DIRS = (
    [(sx, sy, 0) for sx in (1, -1) for sy in (1, -1)]
    + [(sx, 0, sz) for sx in (1, -1) for sz in (1, -1)]
    + [(0, sy, sz) for sy in (1, -1) for sz in (1, -1)]
)

FIRST = []
SECOND = []
for d, (sx, sy, sz) in enumerate(DIRS):
    for k in (0, 1):
        halo = (k == 0) == (sz < 0)
        plane = k if not sz else (k if halo else 1 - k)
        if sx and sy:
            if sx > 0:
                FIRST.append((d, k, "sy", (0 if sy > 0 else 2) + k))
            else:
                SECOND.append((d, k, "yp2" if sy > 0 else "ym2", 2 + k))
        elif sx:
            name = ("sh" if halo else "s") if sx > 0 else ("xh" if halo else "x")
            FIRST.append((d, k, name, plane))
        elif halo:
            SECOND.append((d, k, "yp2" if sy > 0 else "ym2", plane))
        else:
            FIRST.append((d, k, "yp" if sy > 0 else "ym", plane))


def weight_of(direction, spacing):
    length = sum((c * s) ** 2 for c, s in zip(direction, spacing))
    return 1.0 / (4.0 * length)


def dot(a, b):
    return lax.dot_general(a, b, (((1,), (0,)), ((), ())), preferred_element_type=F32)


def left_kernel(order_ref, own_ref, over_ref, out_ref, lhs_ref):
    n = own_ref.shape[-1]

    @pl.when(pl.program_id(0) == 0)
    def _():
        for k in range(2):
            real = own_ref[k, 0].T
            imag = own_ref[k, 1].T
            lhs_ref[k, :n, :n] = real
            lhs_ref[k, :n, n:] = imag
            lhs_ref[k, n:, :n] = -imag
            lhs_ref[k, n:, n:] = real

    for k in range(2):
        rhs = jnp.concatenate([over_ref[0, 0, 0, 0, k], over_ref[0, 1, 0, 0, k]], axis=0)
        res = dot(lhs_ref[k], rhs).astype(BF16)
        out_ref[0, k, 0] = res[:n]
        out_ref[0, k, 1] = res[n:]


def left_products(order, own, over):
    nvec, n = over.shape[0], own.shape[-1]
    return pl.pallas_call(
        left_kernel,
        out_shape=jax.ShapeDtypeStruct((nvec, 2, 2, n, n), BF16),
        grid_spec=pltpu.PrefetchScalarGridSpec(
            num_scalar_prefetch=1,
            grid=(nvec,),
            in_specs=[
                pl.BlockSpec((2, 2, n, n), lambda d, order: (0, 0, 0, 0)),
                pl.BlockSpec((1, 2, 1, 1, 2, n, n), lambda d, order: (order[d], 0, 0, 0, 0, 0, 0)),
            ],
            out_specs=pl.BlockSpec((1, 2, 2, n, n), lambda d, order: (d, 0, 0, 0, 0)),
            scratch_shapes=[pltpu.VMEM((2, 2 * n, 2 * n), BF16)],
        ),
        cost_estimate=pl.CostEstimate(
            flops=nvec * 2 * 8 * n**3, bytes_accessed=nvec * 16 * n * n, transcendentals=0
        ),
        compiler_params=pltpu.CompilerParams(vmem_limit_bytes=12 << 20),
        name="left_products",
    )(order, own, over)


def angle(y, x):
    ax, ay = jnp.abs(x), jnp.abs(y)
    big, small = jnp.maximum(ax, ay), jnp.minimum(ax, ay)
    ratio = small / jnp.where(big == 0.0, 1.0, big)
    upper = ratio > 0.41421356
    z = jnp.where(upper, (ratio - 1.0) / (ratio + 1.0), ratio)
    z2 = z * z
    poly = (8.05374449538e-2 * z2 - 1.38776856032e-1) * z2 + 1.99777106478e-1
    poly = (poly * z2 - 3.33329491539e-1) * z2 * z + z
    res = poly + jnp.where(upper, 0.25 * math.pi, 0.0)
    res = jnp.where(ay > ax, 0.5 * math.pi - res, res)
    res = jnp.where(x < 0.0, math.pi - res, res)
    return jnp.where(y < 0.0, -res, res)


def m_units(units, names, spacing, left_ref, sources, before, m_ref, diag_ref, part_ref):
    n = left_ref.shape[-1]
    half = n // 2
    rows = lax.broadcasted_iota(jnp.int32, (half, half), 0)
    cols = lax.broadcasted_iota(jnp.int32, (half, half), 1)
    eye = rows == cols
    for u, (d, k, name, plane) in enumerate(units):
        source = sources[names.index(name)]
        real, imag = left_ref[d, k, 0], left_ref[d, k, 1]
        lhs = jnp.concatenate(
            [jnp.concatenate([real, -imag], axis=1), jnp.concatenate([imag, real], axis=1)], axis=0
        )
        rhs = jnp.concatenate([source[plane, 0], source[plane, 1]], axis=0)
        res = dot(lhs, rhs)
        m_ref[u, 0] = res[:n]
        m_ref[u, 1] = res[n:]
        for part in range(2):
            for h in range(2):
                block = res[part * n + h * half : part * n + (h + 1) * half, h * half : (h + 1) * half]
                line = jnp.sum(jnp.where(eye, block, 0.0), axis=0, keepdims=True)
                diag_ref[part, u : u + 1, h * half : (h + 1) * half] = line
    real, imag = diag_ref[0], diag_ref[1]
    phase = angle(imag, real)
    diag_ref[2] = phase
    extra = 1.0 - (real * real + imag * imag) + phase * phase
    for row in range(4):
        total = before(row)
        for u, (d, _, _, _) in enumerate(units):
            weight = weight_of(DIRS[d], spacing)
            if row < 3:
                factor = weight * DIRS[d][row] * spacing[row]
                if factor:
                    term = factor * phase[u : u + 1]
                    total = term if total is None else total + term
            else:
                term = weight * extra[u : u + 1]
                total = term if total is None else total + term
        part_ref[row : row + 1] = total


def m_products(units, spacing, left, operands, before):
    names = list(operands)
    n = left.shape[-1]
    count = len(units)

    def kernel(*refs):
        left_ref = refs[0]
        sources = refs[1 : 1 + len(names)]
        if before is None:
            get = lambda row: None
        else:
            get = lambda row: refs[1 + len(names)][row : row + 1]
        m_units(units, names, spacing, left_ref, sources, get, *refs[-3:])

    args = [left] + [operands[name] for name in names] + ([] if before is None else [before])
    vmem = pl.BlockSpec(memory_space=pltpu.VMEM)
    return pl.pallas_call(
        kernel,
        out_shape=(
            jax.ShapeDtypeStruct((count, 2, n, n), F32),
            jax.ShapeDtypeStruct((3, count, n), F32),
            jax.ShapeDtypeStruct((4, n), F32),
        ),
        in_specs=[vmem] * len(args),
        out_specs=(vmem, vmem, vmem),
        cost_estimate=pl.CostEstimate(
            flops=count * 8 * n**3, bytes_accessed=count * 16 * n * n, transcendentals=0
        ),
        name=f"m_products_{count}",
    )(*args)


def split(value):
    high = value.astype(BF16)
    return high, (value - high.astype(F32)).astype(BF16)


def final_kernel(spacing, total_k, sign_ref, m1_ref, d1_ref, m2_ref, d2_ref, sum_ref, gauge_ref,
                 new_ref, centres_ref, spread_ref, t_ref, s_ref, wx_ref, wa_ref, wf_ref):
    n = sum_ref.shape[-1]
    sign = sign_ref[0].astype(F32)
    centre_local = [-(sum_ref[a : a + 1] / total_k) for a in range(3)]
    centre_global = [centre_local[0] * sign, centre_local[1], centre_local[2]]
    squares = centre_local[0] ** 2 + centre_local[1] ** 2 + centre_local[2] ** 2
    for a in range(3):
        centres_ref[a : a + 1] = centre_global[a]
    spread_ref[...] = jnp.sum(sum_ref[3:4] / total_k - squares, axis=1, keepdims=True)

    all_units = [(m1_ref, d1_ref, u, unit) for u, unit in enumerate(FIRST)]
    all_units += [(m2_ref, d2_ref, u, unit) for u, unit in enumerate(SECOND)]
    for i, (_, d_ref, u, unit) in enumerate(all_units):
        direction = DIRS[unit[0]]
        weight = weight_of(direction, spacing)
        real, imag = d_ref[0, u : u + 1], d_ref[1, u : u + 1]
        q = d_ref[2, u : u + 1]
        for a in range(3):
            if direction[a]:
                q = q + (direction[a] * spacing[a]) * centre_local[a]
        t = q / jnp.maximum(real * real + imag * imag, FLOOR)
        s_ref[0, i : i + 1] = weight * (real + imag * t)
        s_ref[1, i : i + 1] = weight * (real * t - imag)

    chunk = 16

    def rows_step(step, carry):
        at = pl.ds(pl.multiple_of(step * chunk, chunk), chunk)
        for k in range(2):
            total_r = total_i = None
            for i, (m_ref, _, u, unit) in enumerate(all_units):
                if unit[1] != k:
                    continue
                mr, mi = m_ref[u, 0, at, :], m_ref[u, 1, at, :]
                sr, si = s_ref[0, i : i + 1], s_ref[1, i : i + 1]
                tr = mr * sr - mi * si
                ti = mr * si + mi * sr
                total_r = tr if total_r is None else total_r + tr
                total_i = ti if total_i is None else total_i + ti
            t_ref[k, 0, at, :] = total_r
            t_ref[k, 1, at, :] = total_i
        return carry

    lax.fori_loop(0, n // chunk, rows_step, 0)

    def put_weights(w_ref, k, value):
        high, low = split(value)
        for j, part in enumerate((high, low)):
            w_ref[k, j, :n] = part
            w_ref[k, j, n:, :n] = -part[:, n:]
            w_ref[k, j, n:, n:] = part[:, :n]
        return high, low

    def product(pair, w_ref, k):
        high, low = pair
        return dot(high, w_ref[k, 0]) + (dot(high, w_ref[k, 1]) + dot(low, w_ref[k, 0]))

    ident_rows = lax.broadcasted_iota(jnp.int32, (n, 2 * n), 0)
    ident_cols = lax.broadcasted_iota(jnp.int32, (n, 2 * n), 1)
    ident = jnp.where(ident_rows == ident_cols, 1.0, 0.0).astype(F32)
    inv = [1.0 / math.factorial(j) for j in range(TERMS + 1)]
    both = range(2)
    x, a2, a3 = [], [], []
    pair = []
    scale = STEP * 2.0
    for k in both:
        real, imag = t_ref[k, 0], t_ref[k, 1]
        x.append(jnp.concatenate([scale * (real - real.T), scale * (imag + imag.T)], axis=1))
        pair.append(put_weights(wx_ref, k, x[k]))
    for k in both:
        a2.append(product(pair[k], wx_ref, k))
    for k in both:
        a3.append(product(split(a2[k]), wx_ref, k))
        put_weights(wa_ref, k, a3[k])
    q = [inv[9] * ident + inv[10] * x[k] + inv[11] * a2[k] + inv[12] * a3[k] for k in both]
    for base in (6, 3, 0):
        q = [
            (inv[base] * ident + inv[base + 1] * x[k] + inv[base + 2] * a2[k])
            + product(split(q[k]), wa_ref, k)
            for k in both
        ]
    for k in both:
        put_weights(wf_ref, k, q[k])
    for k in both:
        gauge = jnp.concatenate([gauge_ref[0, k], gauge_ref[1, k]], axis=1)
        res = product(split(gauge), wf_ref, k)
        new_ref[0, k] = res[:, :n]
        new_ref[1, k] = res[:, n:]


def final_step(spacing, total_k, sign, m1, d1, m2, d2, summed, gauge):
    n = gauge.shape[-1]

    def kernel(*refs):
        final_kernel(spacing, total_k, *refs)

    vmem = pl.BlockSpec(memory_space=pltpu.VMEM)
    return pl.pallas_call(
        kernel,
        out_shape=(
            jax.ShapeDtypeStruct((2, 2, n, n), F32),
            jax.ShapeDtypeStruct((3, n), F32),
            jax.ShapeDtypeStruct((1, 1), F32),
        ),
        in_specs=[pl.BlockSpec(memory_space=pltpu.SMEM)] + [vmem] * 6,
        out_specs=(vmem, vmem, vmem),
        scratch_shapes=[
            pltpu.VMEM((2, 2, n, n), F32),
            pltpu.VMEM((2, len(FIRST) + len(SECOND), n), F32),
            pltpu.VMEM((2, 2, 2 * n, 2 * n), BF16),
            pltpu.VMEM((2, 2, 2 * n, 2 * n), BF16),
            pltpu.VMEM((2, 2, 2 * n, 2 * n), BF16),
        ],
        cost_estimate=pl.CostEstimate(
            flops=2 * 6 * 3 * 8 * n**3, bytes_accessed=4 << 20, transcendentals=0
        ),
        name="final_step",
    )(sign, m1, d1, m2, d2, summed, gauge)


def per_device(offsets, gauge, intersections):
    count_x, count_y = lax.axis_size("kx"), lax.axis_size("ky")
    blocks_z = lax.axis_size("kz")
    depth = gauge.shape[3]
    n = gauge.shape[4]
    assert count_x == 4 and count_y == 4 and blocks_z == 8 and depth == 2
    counts = (count_x, count_y, blocks_z * depth)
    spacing = tuple(2.0 * math.pi / c for c in counts)
    total_k = float(counts[0] * counts[1] * counts[2])

    def moved(value, axis, pairs):
        return lax.ppermute(value, axis, pairs)

    def along(value, axis, step):
        size = lax.axis_size(axis)
        return moved(value, axis, [((i + step) % size, i) for i in range(size)])

    def sibling(value):
        return moved(value, "kx", [(i, i ^ 1) for i in range(4)])

    def across(value):
        return moved(value, "kx", [(i, 3 - i) for i in range(4)])

    gauge = gauge[:, 0, 0]
    own = jnp.swapaxes(gauge, 0, 1).astype(BF16)

    zm = along(own[1:2], "kz", -1)
    zp = along(own[0:1], "kz", 1)
    x = across(own)
    yp = along(own, "ky", 1)
    ym = along(own, "ky", -1)
    s = sibling(own)
    halo = jnp.concatenate([zm, zp])
    more = jnp.concatenate([halo, x])
    yp2 = along(more, "ky", 1)
    ym2 = along(more, "ky", -1)
    xh = across(halo)
    sh = sibling(halo)
    sy = sibling(jnp.concatenate([yp, ym]))

    sign = 1 - 2 * (lax.axis_index("kx") & 1)
    local = offsets * jnp.stack([sign, jnp.int32(1), jnp.int32(1)])
    code = local[:, 0] * 9 + local[:, 1] * 3 + local[:, 2]
    wanted = jnp.array([9 * a + 3 * b + c for a, b, c in DIRS], jnp.int32)
    order = jnp.argmax(code[None, :] == wanted[:, None], axis=1).astype(jnp.int32)

    left = left_products(order, own, intersections)
    m1, d1, part1 = m_products(
        FIRST, spacing, left, dict(sy=sy, s=s, x=x, sh=sh, xh=xh, yp=yp, ym=ym), None
    )
    m2, d2, part = m_products(SECOND, spacing, left, dict(yp2=yp2, ym2=ym2), part1)

    signs = jnp.concatenate([sign.reshape(1, 1), jnp.ones((3, 1), jnp.int32)]).astype(F32)
    total = part * signs
    total = total + sibling(total)
    total = total + across(total)
    for flip in (1, 3):
        total = total + moved(total, "ky", [(i, i ^ flip) for i in range(4)])
    for flip in (1, 3):
        total = total + moved(total, "kz", [(i, i ^ flip) for i in range(8)])
    total = total + moved(
        total, ("kx", "kz"), [(i * 8 + j, (i ^ 2) * 8 + (j ^ 4)) for i in range(4) for j in range(8)]
    )
    new, centres, spread = final_step(
        spacing, total_k, sign.reshape(1), m1, d1, m2, d2, total * signs, gauge
    )
    return new.reshape(2, 1, 1, depth, n, n), centres, spread.reshape(())


def solution(mesh):
    gauge_spec = P(None, "kx", "ky", "kz", None, None)
    return jax.shard_map(
        per_device,
        mesh=mesh,
        in_specs=(P(), gauge_spec, P(None, None, "kx", "ky", "kz", None, None)),
        out_specs=(gauge_spec, P(), P()),
        check_vma=False,
    )
```
